32 devices in a mesh: leaf: 16 (over z, y, core), top: 2 (over x).
Axes of the slice: x: 2, y: 2, z: 4, core: 2. Of those that a mesh axis runs over, the one named last changes fastest.
Arguments:
- vectors: bfloat16 [2, 16, 768, 512], P('top', 'leaf'), may hold values from -6 to 6
- near_tiles: bfloat16 [2, 16, 8, 768, 768], P('top', 'leaf'), may hold values from -0.078125 to 0.078125
- leaf_basis: bfloat16 [2, 16, 768, 128], P('top', 'leaf'), may hold values from -0.21875 to 0.21875
- transfer: bfloat16 [2, 16, 128, 128], P('top', 'leaf'), may hold values from -0.25 to 0.25
- coupling: bfloat16 [2, 16, 7, 128, 128], P('top', 'leaf'), may hold values from -0.1875 to 0.1875
- top_coupling: bfloat16 [2, 2, 128, 128], P('top'), may hold values from -0.375 to 0.375
- near_list: int32 [2, 16, 8], P('top', 'leaf'), may hold values from -4 to 4, as said below
- far_list: int32 [2, 16, 7], P('top', 'leaf'), may hold values from 0 to 15, as said below
- row_counts: int32 [2, 16], P('top', 'leaf'), may hold values from 384 to 768
Outputs:
- product: float32 [2, 16, 768, 512], P('top', 'leaf')
The draws below stay inside these ranges and needn't reach their ends.
Inputs may be any that keep to these rules, and one draw needn't show every extreme that they name: `near_list`: each leaf's 8 offsets are distinct; an offset that leads outside the cluster's 16 leaves stands for an absent block. `far_list`: each leaf's entries are distinct positions in its cluster, each more than 4 away from the leaf's own position. `row_counts`: rows at and beyond the count are padding.
All inputs are finite; a program needn't handle non-finite values.
Results may differ from the reference program's by a relative error of at most 0.0045.
Values may be sent and summed in bfloat16 or wider, within the bound.
A program may use at most 128 MiB of HBM per device.

```python
import jax
import jax.numpy as jnp
from jax import lax

LEAF_ROWS = 768
RANK = 128
VECS = 512
REACH = 4
NEAR = 8
FAR = 7
CLUSTERS = 2
GROUP = 16
TOPFAR = 2


def draw_near_list(key, part):
    subkeys = jax.random.split(key, CLUSTERS * GROUP)
    orders = jax.vmap(lambda single: jax.random.permutation(single, 2 * REACH + 1))(subkeys)
    return (orders[:, :NEAR] - REACH).astype(jnp.int32).reshape(CLUSTERS, GROUP, NEAR)


def draw_far_list(key, part):
    scores = jax.random.randint(jax.random.fold_in(key, 7), (CLUSTERS, GROUP, GROUP), 0, 1 << 20)
    column = jnp.arange(GROUP, dtype=jnp.int32)
    scores = scores * GROUP + column[None, None, :]
    distance = jnp.abs(column[:, None] - column[None, :])
    scores = jnp.where(distance[None] > REACH, scores, -1)
    values, picked = lax.top_k(scores, FAR)
    return picked.astype(jnp.int32)


def touch_ends(result, stream_key, smallest, high):
    index_at = [jax.random.randint(jax.random.fold_in(stream_key, axis), (), 0, length) for axis, length in enumerate(result.shape)]
    widest = result.shape.index(max(result.shape))
    beside = index_at[:widest] + [(index_at[widest] + 1) % result.shape[widest]] + index_at[widest + 1:]
    return result.at[tuple(index_at)].set(smallest).at[tuple(beside)].set(high)


def shard_levels(own_key, extent, shards, smallest, high):
    gain, own = 1.0, jax.random.fold_in(own_key, 6)
    for dim, blocks in shards:
        heights = jnp.exp(jax.random.uniform(jax.random.fold_in(own, dim), (blocks,), jnp.float32, smallest / len(shards), high / len(shards)))
        gain = gain * jnp.repeat(heights, extent[dim] // blocks).reshape([-1 if axis == dim else 1 for axis in range(len(extent))])
    return gain


def normal_values(stream_key, extent, width, most, cuts=(), kind=jnp.bfloat16):
    factor_of = shard_levels(stream_key, extent, cuts, -0.22, 0.18) if cuts else 1.0
    result = jax.random.normal(stream_key, extent, jnp.float32) * width * factor_of
    return jnp.minimum(jnp.maximum(result, -most), most).astype(kind)


def setup_inputs(seed: int = 0) -> dict:
    streams_of = jax.random.split(jax.random.key(seed), 10)
    vectors = normal_values(streams_of[0], (CLUSTERS, GROUP, LEAF_ROWS, VECS), 1.0, 6.0, ((0, 2), (1, 16)))
    near_tiles = normal_values(streams_of[1], (CLUSTERS, GROUP, NEAR, LEAF_ROWS, LEAF_ROWS), (NEAR * LEAF_ROWS) ** -0.5, 0.078125, ((0, 2), (1, 16)))
    leaf_basis = normal_values(streams_of[2], (CLUSTERS, GROUP, LEAF_ROWS, RANK), LEAF_ROWS ** -0.5, 0.21875, ((0, 2), (1, 16)))
    transfer = normal_values(streams_of[3], (CLUSTERS, GROUP, RANK, RANK), (RANK * 4) ** -0.5, 0.25, ((0, 2), (1, 16)))
    coupling = normal_values(streams_of[4], (CLUSTERS, GROUP, FAR, RANK, RANK), (RANK * FAR) ** -0.5, 0.1875, ((0, 2), (1, 16)))
    top_coupling = normal_values(streams_of[5], (CLUSTERS, TOPFAR, RANK, RANK), (RANK * TOPFAR) ** -0.5, 0.375, ((0, 2),))
    near_list = draw_near_list(jax.random.fold_in(streams_of[9], 71), 0)
    far_list = draw_far_list(jax.random.fold_in(streams_of[9], 71), 0)
    row_counts = touch_ends(jax.random.randint(streams_of[8], (CLUSTERS, GROUP), LEAF_ROWS // 2, LEAF_ROWS + 1), jax.random.fold_in(streams_of[8], 1), LEAF_ROWS // 2, LEAF_ROWS).astype(jnp.int32)
    return {"vectors": vectors, "near_tiles": near_tiles, "leaf_basis": leaf_basis, "transfer": transfer, "coupling": coupling, "top_coupling": top_coupling, "near_list": near_list, "far_list": far_list, "row_counts": row_counts}


def reference(vectors, near_tiles, leaf_basis, transfer, coupling, top_coupling, near_list, far_list, row_counts):
    row_index = jnp.arange(LEAF_ROWS, dtype=jnp.int32)
    keep = (row_index[None, None, :] < row_counts[:, :, None]).astype(jnp.bfloat16)
    masked = vectors * keep[..., None]

    def near_leaf(index):
        cluster = index // GROUP
        member = index % GROUP
        targets = member + near_list[cluster, member]
        valid = ((targets >= 0) & (targets < GROUP)).astype(jnp.bfloat16)
        safe = jnp.clip(targets, 0, GROUP - 1).astype(jnp.int32)
        sources = masked[cluster][safe] * valid[:, None, None]
        return jnp.einsum("kij,kjv->iv", near_tiles[cluster, member].astype(jnp.float32), sources.astype(jnp.float32))

    near = lax.map(near_leaf, jnp.arange(CLUSTERS * GROUP, dtype=jnp.int32))
    near = near.reshape(CLUSTERS, GROUP, LEAF_ROWS, VECS)

    basis = leaf_basis.astype(jnp.float32)
    nested = transfer.astype(jnp.float32)
    coeff = jnp.einsum("cgir,cgiv->cgrv", basis, masked.astype(jnp.float32)).astype(jnp.bfloat16)
    upward = jnp.einsum("cgab,cgav->cgbv", nested, coeff.astype(jnp.float32))
    parent = jnp.sum(upward, axis=1).astype(jnp.bfloat16)
    cluster_ids = jnp.arange(CLUSTERS, dtype=jnp.int32)
    sibling_ids = (cluster_ids[:, None] + 1 + jnp.arange(TOPFAR, dtype=jnp.int32)[None, :]) % CLUSTERS
    chosen = parent[sibling_ids]
    parent_field = jnp.einsum("cmab,cmbv->cav", top_coupling.astype(jnp.float32), chosen.astype(jnp.float32)).astype(jnp.bfloat16)
    cluster_index = cluster_ids[:, None, None]
    siblings = coeff[cluster_index, far_list]
    local_field = jnp.einsum("cgmab,cgmbv->cgav", coupling.astype(jnp.float32), siblings.astype(jnp.float32))
    local_field = local_field + jnp.einsum("cgab,cbv->cgav", nested, parent_field.astype(jnp.float32))
    local_field = local_field.astype(jnp.bfloat16)
    far = jnp.einsum("cgir,cgrv->cgiv", basis, local_field.astype(jnp.float32))
    return (near + far) * keep[..., None].astype(jnp.float32)
```

```python
import functools

import jax
import jax.numpy as jnp
from jax import lax
from jax.experimental import pallas as pl
from jax.experimental.pallas import tpu as pltpu
from jax.sharding import PartitionSpec as P

REACH = 4


def mirrored(index, bits):
    total = 0
    for bit in range(bits):
        total = total + lax.rem(lax.div(index, 1 << bit), 2) * (1 << (bits - 1 - bit))
    return total


def kernel(
    leaves,
    clusters,
    masked_ref,
    packed_ref,
    window,
    gathered,
    parents,
    send_sem,
    recv_sem,
    step_send,
    step_recv,
    top_send,
    top_recv,
    own_sem,
    same_sem,
):
    me = lax.axis_index("leaf")
    cluster = lax.axis_index("top")
    core = lax.rem(me, 2)
    toward = 1 - 2 * core
    partner = me + toward
    bits = leaves.bit_length() - 1
    vecs = masked_ref.shape[1]
    rank = packed_ref.shape[0]
    spot = mirrored(me, bits)

    own = pltpu.make_async_copy(
        packed_ref, gathered.at[pl.ds(pl.multiple_of(spot * rank, rank), rank)], own_sem
    )
    own.start()
    same = pltpu.make_async_copy(masked_ref, window.at[REACH], same_sem)
    same.start()

    def inside(offset):
        return jnp.logical_and(me + offset >= 0, me + offset < leaves)

    def peer_of(step):
        stride = leaves >> (step + 1)
        return me + stride * (1 - 2 * lax.rem(lax.div(me, stride), 2))

    barrier = pltpu.get_barrier_semaphore()
    expected = bits + clusters - 1
    for offset in (2, -2, 4, -4):
        expected = expected + inside(offset).astype(jnp.int32)

        @pl.when(inside(offset))
        def _(offset=offset):
            pl.semaphore_signal(
                barrier, inc=1, device_id={"leaf": me + offset}, device_id_type=pl.DeviceIdType.MESH
            )

    for step in range(bits):
        pl.semaphore_signal(
            barrier, inc=1, device_id={"leaf": peer_of(step)}, device_id_type=pl.DeviceIdType.MESH
        )
    for shift in range(1, clusters):
        pl.semaphore_signal(
            barrier,
            inc=1,
            device_id={"top": lax.rem(cluster + shift, clusters)},
            device_id_type=pl.DeviceIdType.MESH,
        )
    pl.semaphore_wait(barrier, expected)

    def exchange(step):
        size = 1 << step
        start = lax.div(spot, size) * size
        block = gathered.at[pl.ds(pl.multiple_of(start * rank, rank), size * rank)]
        return pltpu.make_async_remote_copy(
            src_ref=block,
            dst_ref=block,
            send_sem=step_send.at[step],
            recv_sem=step_recv.at[step],
            device_id={"leaf": peer_of(step)},
            device_id_type=pl.DeviceIdType.MESH,
        )

    def direct(offset):
        return pltpu.make_async_remote_copy(
            src_ref=masked_ref,
            dst_ref=window.at[REACH - offset],
            send_sem=send_sem.at[REACH + offset],
            recv_sem=recv_sem.at[REACH - offset],
            device_id={"leaf": me + offset},
            device_id_type=pl.DeviceIdType.MESH,
        )

    def forward(offset, slot):
        return pltpu.make_async_remote_copy(
            src_ref=masked_ref if offset == 0 else window.at[REACH + offset],
            dst_ref=window.at[REACH + offset - toward],
            send_sem=send_sem.at[slot],
            recv_sem=recv_sem.at[REACH + offset - toward],
            device_id={"leaf": partner},
            device_id_type=pl.DeviceIdType.MESH,
        )

    def forwarded(offset):
        if offset == 4:
            return jnp.logical_and(inside(offset), core == 0)
        if offset == -4:
            return jnp.logical_and(inside(offset), core == 1)
        return inside(offset)

    slot_of = {0: 1, 2: 3, -2: 5, 4: 7, -4: 4}

    def arrival(offset):
        block = window.at[REACH + offset]
        return pltpu.make_async_remote_copy(
            src_ref=block,
            dst_ref=block,
            send_sem=send_sem.at[REACH + offset],
            recv_sem=recv_sem.at[REACH + offset],
            device_id={"leaf": partner},
            device_id_type=pl.DeviceIdType.MESH,
        )

    own.wait()
    exchange(0).start()
    forward(0, slot_of[0]).start()
    for offset in (2, -2):

        @pl.when(inside(offset))
        def _(offset=offset):
            direct(offset).start()

    exchange(0).wait_recv()
    exchange(1).start()
    for offset in (4, -4):

        @pl.when(inside(offset))
        def _(offset=offset):
            direct(offset).start()

    exchange(1).wait_recv()
    exchange(2).start()
    for offset in (2, -2):

        @pl.when(inside(offset))
        def _(offset=offset):
            direct(-offset).wait_recv()
            forward(offset, slot_of[offset]).start()

    for step in range(2, bits):
        exchange(step).wait_recv()
        if step + 1 < bits:
            exchange(step + 1).start()

    def contract(left, right):
        return lax.dot_general(
            left, right, (((0,), (0,)), ((), ())), preferred_element_type=jnp.float32
        )

    parent = contract(gathered[:, vecs:], gathered[:, :vecs]).astype(jnp.bfloat16)
    parents[cluster] = parent

    for offset in (4, -4):

        @pl.when(inside(offset))
        def _(offset=offset):
            direct(-offset).wait_recv()

        @pl.when(forwarded(offset))
        def _(offset=offset):
            forward(offset, slot_of[offset]).start()

    def share(shift):
        return pltpu.make_async_remote_copy(
            src_ref=parents.at[cluster],
            dst_ref=parents.at[cluster],
            send_sem=top_send.at[shift],
            recv_sem=top_recv.at[shift],
            device_id={"top": lax.rem(cluster + shift, clusters)},
            device_id_type=pl.DeviceIdType.MESH,
        )

    for shift in range(1, clusters):
        share(shift).start()

    for offset in (1, -1, 3, -3):

        @pl.when(inside(offset))
        def _(offset=offset):
            arrival(offset).wait_recv()

    for shift in range(1, clusters):
        share(shift).wait_recv()
    same.wait()
    for step in range(bits):
        exchange(step).wait_send()
    for shift in range(1, clusters):
        share(shift).wait_send()
    for offset in (2, -2, 4, -4):

        @pl.when(inside(offset))
        def _(offset=offset):
            direct(offset).wait_send()

    for offset in (0, 2, -2, 4, -4):

        @pl.when(forwarded(offset))
        def _(offset=offset):
            forward(offset, slot_of[offset]).wait_send()


def local_kernel(
    clusters,
    slots,
    valid,
    places,
    scalars,
    tile_ref,
    source_ref,
    gathered,
    parents,
    basis_ref,
    nested_ref,
    coupling_ref,
    top_ref,
    out_ref,
):
    k = pl.program_id(0)
    rows, vecs = out_ref.shape
    rank = nested_ref.shape[0]
    part = rows // 3 if rows % 3 == 0 else rows

    @pl.when(k == 0)
    def _():
        out_ref[...] = jnp.zeros_like(out_ref)

    @pl.when(valid[k] == 1)
    def _():
        def piece(index, carry):
            span = pl.ds(pl.multiple_of(index * part, part), part)
            out_ref[span, :] += jnp.dot(
                tile_ref[0, span, :], source_ref[0], preferred_element_type=jnp.float32
            )
            return carry

        lax.fori_loop(0, rows // part, piece, 0)

    @pl.when(k == pl.num_programs(0) - 1)
    def _():
        field = jnp.zeros((rank, vecs), jnp.float32)
        for m in range(coupling_ref.shape[0]):
            start = pl.multiple_of(places[m] * rank, rank)
            field = field + jnp.dot(
                coupling_ref[m],
                gathered[pl.ds(start, rank), :vecs],
                preferred_element_type=jnp.float32,
            )
        above = jnp.zeros((rank, vecs), jnp.float32)
        for m in range(top_ref.shape[0]):
            above = above + jnp.dot(
                top_ref[m],
                parents[lax.rem(scalars[1] + 1 + m, clusters)],
                preferred_element_type=jnp.float32,
            )
        field = field + jnp.dot(
            nested_ref[...], above.astype(jnp.bfloat16), preferred_element_type=jnp.float32
        )
        far = jnp.dot(
            basis_ref[...], field.astype(jnp.bfloat16), preferred_element_type=jnp.float32
        )
        row = lax.broadcasted_iota(jnp.int32, (rows, vecs), 0)
        out_ref[...] = jnp.where(row < scalars[0], out_ref[...] + far, 0.0)


def body(
    vectors,
    near_tiles,
    leaf_basis,
    transfer,
    coupling,
    top_coupling,
    near_list,
    far_list,
    row_counts,
):
    leaves = lax.axis_size("leaf")
    clusters = lax.axis_size("top")
    rows, vecs = vectors.shape[2:]
    keep = (jnp.arange(rows, dtype=jnp.int32) < row_counts[0, 0]).astype(jnp.bfloat16)
    masked = vectors[0, 0] * keep[:, None]
    basis = leaf_basis[0, 0]
    nested = transfer[0, 0]
    rank = nested.shape[0]
    coeff = jnp.einsum("ir,iv->rv", basis, masked, preferred_element_type=jnp.float32).astype(
        jnp.bfloat16
    )
    packed = jnp.concatenate([coeff, nested], axis=1)
    tiles = near_tiles[0, 0]
    bits = leaves.bit_length() - 1
    span = 2 * REACH + 1
    vmem = pl.BlockSpec(memory_space=pltpu.VMEM)
    window, gathered, parents = pl.pallas_call(
        functools.partial(kernel, leaves, clusters),
        out_shape=(
            jax.ShapeDtypeStruct((span, rows, vecs), jnp.bfloat16),
            jax.ShapeDtypeStruct((leaves * rank, vecs + rank), jnp.bfloat16),
            jax.ShapeDtypeStruct((clusters, rank, vecs), jnp.bfloat16),
        ),
        in_specs=[vmem, vmem],
        out_specs=(pl.BlockSpec(memory_space=pl.ANY), vmem, vmem),
        scratch_shapes=[
            pltpu.SemaphoreType.DMA((span,)),
            pltpu.SemaphoreType.DMA((span,)),
            pltpu.SemaphoreType.DMA((bits,)),
            pltpu.SemaphoreType.DMA((bits,)),
            pltpu.SemaphoreType.DMA((clusters,)),
            pltpu.SemaphoreType.DMA((clusters,)),
            pltpu.SemaphoreType.DMA,
            pltpu.SemaphoreType.DMA,
        ],
        compiler_params=pltpu.CompilerParams(
            collective_id=0, has_side_effects=True, vmem_limit_bytes=24 * 1024 * 1024
        ),
        cost_estimate=pl.CostEstimate(
            flops=2 * leaves * rank * rank * vecs,
            bytes_accessed=16 * span * rows * vecs,
            transcendentals=0,
        ),
    )(masked, packed)
    me = lax.axis_index("leaf")
    offsets = near_list[0, 0]
    valid = (me + offsets >= 0) & (me + offsets < leaves)
    slots = jnp.where(valid, offsets + REACH, REACH)
    places = mirrored(far_list[0, 0], bits)
    scalars = jnp.stack([row_counts[0, 0], lax.axis_index("top")]).astype(jnp.int32)

    def whole(array):
        return pl.BlockSpec(array.shape, lambda k, *_: (0,) * array.ndim)

    rest = (gathered, parents, basis, nested, coupling[0, 0], top_coupling[0])
    result = pl.pallas_call(
        functools.partial(local_kernel, clusters),
        out_shape=jax.ShapeDtypeStruct((rows, vecs), jnp.float32),
        grid_spec=pltpu.PrefetchScalarGridSpec(
            num_scalar_prefetch=4,
            grid=(tiles.shape[0],),
            in_specs=[
                pl.BlockSpec((1, rows, rows), lambda k, *_: (k, 0, 0)),
                pl.BlockSpec((1, rows, vecs), lambda k, slots, *_: (slots[k], 0, 0)),
            ]
            + [whole(array) for array in rest],
            out_specs=pl.BlockSpec((rows, vecs), lambda k, *_: (0, 0)),
        ),
        compiler_params=pltpu.CompilerParams(
            dimension_semantics=("arbitrary",), vmem_limit_bytes=32 * 1024 * 1024
        ),
    )(slots, valid.astype(jnp.int32), places, scalars, tiles, window, *rest)
    return result[None, None]


def solution(mesh):
    in_specs = (
        P("top", "leaf", None, None),
        P("top", "leaf", None, None, None),
        P("top", "leaf", None, None),
        P("top", "leaf", None, None),
        P("top", "leaf", None, None, None),
        P("top", None, None, None),
        P("top", "leaf", None),
        P("top", "leaf", None),
        P("top", "leaf"),
    )
    out_specs = P("top", "leaf", None, None)
    return jax.shard_map(body, mesh=mesh, in_specs=in_specs, out_specs=out_specs, check_vma=False)
```
